32 devices in a mesh: rep: 8 (over y, x, core), tp: 4 (over z).
Axes of the slice: x: 2, y: 2, z: 4, core: 2. Of those that a mesh axis runs over, the one named last changes fastest.
Arguments:
- flat_buffer: bfloat16 [578912256], P(('rep', 'tp')), may hold values from -60 to 60
- shard_pad: int32 [2, 6], replicated, may hold values from 0 to 2
Outputs:
- q_served: bfloat16 [2, 6144, 6144], P(None, 'rep', 'tp')
- q_scale: float32 [2, 48, 6144], P(None, 'rep', 'tp')
- k_served: bfloat16 [2, 6144, 1024], P(None, 'rep', 'tp')
- k_scale: float32 [2, 48, 1024], P(None, 'rep', 'tp')
- v_served: bfloat16 [2, 6144, 1024], P(None, 'rep', 'tp')
- v_scale: float32 [2, 48, 1024], P(None, 'rep', 'tp')
- o_served: bfloat16 [2, 6144, 6144], P(None, 'tp', 'rep')
- o_scale: float32 [2, 48, 6144], P(None, 'tp', 'rep')
- gate_served: bfloat16 [2, 6144, 16384], P(None, 'rep', 'tp')
- gate_scale: float32 [2, 48, 16384], P(None, 'rep', 'tp')
- up_served: bfloat16 [2, 6144, 16384], P(None, 'rep', 'tp')
- up_scale: float32 [2, 48, 16384], P(None, 'rep', 'tp')
The draws below stay inside these ranges and needn't reach their ends.
All inputs are finite; a program needn't handle non-finite values. Where the reference program divides by a largest or mean magnitude, that divisor is 1e-20 or more.
Results may differ from the reference program's by a relative error of at most 0.001.
Values may be sent and summed in bfloat16 or wider, within the bound.
A program may use at most 192 MiB of HBM per device.

```python
import math
import jax
import jax.numpy as jnp
from jax import lax

D = 6144
KV = 1024
FF = 16384
GROUP = 128
LAYERS = 2
PADMAX = 2
FLAT_DEV = 18091008
FLAT = 578912256
DEVICES = 32


def draw_flat_buffer(key, part):
    first, second = jax.random.split(jax.random.fold_in(key, 17))
    base = jnp.clip(jax.random.normal(first, (FLAT,), jnp.float32), -6.0, 6.0)
    factor = jnp.exp(jax.random.uniform(second, (FLAT // 32,), jnp.float32, 0.0, math.log(10.0)))
    return (base * jnp.repeat(factor, 32)).astype(jnp.bfloat16)


def touch_ends(result, rng, low, high):
    longest = result.shape.index(max(result.shape))
    spots = []
    for shift in (0, 1):
        where = [jax.random.randint(jax.random.fold_in(rng, axis), (), 0, length) for axis, length in enumerate(result.shape)]
        where[longest] = (where[longest] + shift) % result.shape[longest]
        spots.append(tuple(where))
    return result.at[spots[0]].set(low).at[spots[1]].set(high)


def setup_inputs(seed: int = 0) -> dict:
    streams_of = jax.random.split(jax.random.key(seed), 3)
    flat_buffer = draw_flat_buffer(jax.random.fold_in(streams_of[2], 71), 0)
    shard_pad = touch_ends(jax.random.randint(streams_of[1], (LAYERS, 6), 0, PADMAX + 1), jax.random.fold_in(streams_of[1], 1), 0, PADMAX).astype(jnp.int32)
    return {"flat_buffer": flat_buffer, "shard_pad": shard_pad}


def quantize(served):
    values = served.astype(jnp.float32)
    grouped = values.reshape(values.shape[0] // GROUP, GROUP, values.shape[1])
    peak = jnp.max(jnp.abs(grouped), axis=1) + 1e-6
    scaled = (grouped / peak[:, None, :]).astype(jnp.bfloat16)
    return scaled.reshape(served.shape), peak


def reference(flat_buffer, shard_pad):
    widths = (D, KV, KV, D, FF, FF)
    table = flat_buffer.reshape(DEVICES, FLAT_DEV)
    offset = jnp.zeros((), jnp.int32)
    served_all = [[] for index in range(6)]
    scale_all = [[] for index in range(6)]
    for layer in range(LAYERS):
        for index in range(6):
            length = widths[index] // DEVICES * D
            piece = lax.dynamic_slice_in_dim(table, offset.astype(jnp.int32), length, 1)
            whole = piece.reshape(widths[index], D)
            scaled, peak = quantize(whole.T)
            served_all[index].append(scaled)
            scale_all[index].append(peak)
            offset = (offset + length + 128 * shard_pad[layer, index]).astype(jnp.int32)
    outputs = []
    for index in range(6):
        outputs.append(jnp.stack(served_all[index]))
        outputs.append(jnp.stack(scale_all[index]))
    return (outputs[0], outputs[1], outputs[2], outputs[3], outputs[4], outputs[5],
            outputs[6], outputs[7], outputs[8], outputs[9], outputs[10], outputs[11])
```

```python
import functools

import jax
import jax.numpy as jnp
from jax import lax
from jax.experimental import pallas as pl
from jax.experimental.pallas import tpu as pltpu
from jax.sharding import PartitionSpec as P

D = 6144
KV = 1024
FF = 16384
GROUP = 128
LAYERS = 2


def quantize_kernel(order, *refs):
    received, scaled, scale = refs[0], refs[-2], refs[-1]
    group = pl.program_id(0)
    parts = [received[where + (0,)].astype(jnp.float32) for where in order]
    served = jnp.concatenate(parts, axis=0).T
    peak = jnp.max(jnp.abs(served), axis=0, keepdims=True) + 1e-06
    scaled[0] = (served / peak).astype(jnp.bfloat16)
    scale[0, pl.ds(group, 1), :] = peak


def quantize(received, layer, earlier):
    lead = received.shape[:-3]
    groups, rows, width = received.shape[-3:]
    if len(lead) == 2:
        order = [(inner, outer) for outer in range(lead[1]) for inner in range(lead[0])]
    else:
        order = [(inner,) for inner in range(lead[0])]
    total = len(order) * rows
    block = lead + (1, rows, width)
    zeros = (0,) * len(lead)
    return pl.pallas_call(
        functools.partial(quantize_kernel, order),
        grid=(groups,),
        in_specs=[pl.BlockSpec(block, lambda g: zeros + (g, 0, 0))]
        + [pl.BlockSpec(memory_space=pl.ANY)] * len(earlier),
        out_specs=[
            pl.BlockSpec((1, GROUP, total), lambda g: (layer, g, 0)),
            pl.BlockSpec((1, groups, total), lambda g: (layer, 0, 0)),
        ],
        out_shape=[
            jax.ShapeDtypeStruct((LAYERS, groups * GROUP, total), jnp.bfloat16),
            jax.ShapeDtypeStruct((LAYERS, groups, total), jnp.float32),
        ],
        input_output_aliases={1 + i: i for i in range(len(earlier))},
        cost_estimate=pl.CostEstimate(
            flops=20 * groups * GROUP * total,
            bytes_accessed=4 * groups * GROUP * total,
            transcendentals=0,
        ),
    )(received, *earlier)


def on_device(flat_buffer, shard_pad):
    reps = lax.axis_size("rep")
    tps = lax.axis_size("tp")
    devices = reps * tps
    widths = (D, KV, KV, D, FF, FF)
    tiled = flat_buffer.reshape(flat_buffer.shape[0] // GROUP, GROUP)
    offsets = []
    offset = jnp.zeros((), jnp.int32)
    for layer in range(LAYERS):
        for index in range(6):
            offsets.append(offset)
            offset = offset + widths[index] // devices * D // GROUP + shard_pad[layer, index]
    outputs = [()] * 6
    for layer in range(LAYERS):
        for index in (4, 5, 0, 3, 1, 2):
            rows = widths[index] // devices
            lines = D // GROUP
            taken = lax.dynamic_slice_in_dim(tiled, offsets[layer * 6 + index], rows * lines, 0)
            piece = taken.reshape(rows, lines, GROUP).transpose(1, 0, 2)
            if index == 3:
                received = lax.all_to_all(piece, "tp", split_axis=0, concat_axis=0, tiled=True)
                received = received.reshape(tps, lines // tps, rows, GROUP)
            else:
                received = lax.all_to_all(piece, "rep", split_axis=0, concat_axis=0, tiled=True)
                received = received.reshape(reps, lines // reps, rows, GROUP)
                received = lax.all_to_all(received, "tp", split_axis=0, concat_axis=0, tiled=True)
                received = received.reshape(tps, reps // tps, lines // reps, rows, GROUP)
            outputs[index] = quantize(received, layer, tuple(outputs[index]))
    return tuple(array for pair in outputs for array in pair)


def solution(mesh):
    column = P(None, "rep", "tp")
    row = P(None, "tp", "rep")
    return jax.shard_map(
        on_device,
        mesh=mesh,
        in_specs=(P(("rep", "tp")), P()),
        out_specs=(column,) * 6 + (row,) * 2 + (column,) * 4,
        check_vma=False,
    )
```
